256 devices in a mesh: ka: 8 (over y, x_lo), ga: 32 (over x_hi, z, core).
Axes of the slice: x: 4 (x_hi: 2, x_lo: 2; x = x_hi * 2 + x_lo), y: 4, z: 8, core: 2. Of those that a mesh axis runs over, the one named last changes fastest.
Arguments:
- coeffs: bfloat16 [8, 1, 65536, 2, 512], P('ka', None, 'ga'), may hold values from -0.5 to 0.5
- counts: int32 [8, 1], replicated, may hold values from 32768 to 65536
- block_map: int32 [8, 1, 2048], replicated, may hold values from 0 to 2047, as said below
- wrap: int32 [8, 1, 2048], replicated, may hold values from 0 to 31
Outputs:
- margins: float32 [8, 512, 1, 2, 512], P('ka', 'ga')
The draws below stay inside these ranges and needn't reach their ends.
Inputs may be any that keep to these rules, and one draw needn't show every extreme that they name: For each k-point and line, block_map is a permutation of the 2048 blocks. Counting G-shards as runs of 64 blocks, at most 3 blocks of one shard have their partner blocks in any one shard, and for each k-point and line some pair of shards reaches 3.
All inputs are finite; a program needn't handle non-finite values.
Results may differ from the reference program's by a relative error of at most 0.0003.
Values may be sent and summed in bfloat16 or wider, within the bound.
A program may use at most 64 MiB of HBM per device.

```python
import jax
import jax.numpy as jnp
from jax import lax

NB = 512
NPW = 65536
BLK = 32
LINES = 1
NK = 8
NBLK = 2048
BPD = 64
CAP = 3
N_GA = 32


def draw_block_map(key, part):
    shard_count = N_GA
    quarter = shard_count // 4
    line_keys = jax.random.split(jax.random.fold_in(key, 17), NK * LINES)

    def single_map(line_key):
        key_offsets, key_source, key_target = jax.random.split(line_key, 3)
        offsets = jax.random.permutation(key_offsets, shard_count)
        rank_ids = jnp.arange(shard_count, dtype=jnp.int32)
        level_mult = jnp.where(rank_ids < quarter, CAP, jnp.where(rank_ids < 2 * quarter, CAP - 2, CAP - 1)).astype(jnp.int32)
        multiplicity = jnp.zeros((shard_count,), jnp.int32).at[offsets].set(level_mult)
        cum_end = jnp.cumsum(multiplicity)
        slot_ids = jnp.arange(BPD, dtype=jnp.int32)
        offset_index = jnp.sum((slot_ids[:, None] >= cum_end[None, :]).astype(jnp.int32), axis=1)
        target_ids = jnp.arange(shard_count, dtype=jnp.int32)
        source_ids = (target_ids[:, None] + offset_index[None, :]) % shard_count
        source_perm = jax.vmap(lambda sub_key: jax.random.permutation(sub_key, BPD))(jax.random.split(key_source, shard_count)).astype(jnp.int32)
        target_perm = jax.vmap(lambda sub_key: jax.random.permutation(sub_key, BPD))(jax.random.split(key_target, shard_count)).astype(jnp.int32)
        values = source_ids * BPD + source_perm[source_ids, slot_ids[None, :]]
        write_at = target_ids[:, None] * BPD + target_perm
        return jnp.zeros((NBLK,), jnp.int32).at[write_at.reshape(-1)].set(values.reshape(-1).astype(jnp.int32))
    return jax.vmap(single_map)(line_keys).reshape(NK, LINES, NBLK).astype(jnp.int32)


def touch_ends(array, own_key, low, top_value):
    spot = [jax.random.randint(jax.random.fold_in(own_key, axis), (), 0, length) for axis, length in enumerate(array.shape)]
    longest = array.shape.index(max(array.shape))
    next_to = spot[:longest] + [(spot[longest] + 1) % array.shape[longest]] + spot[longest + 1:]
    return array.at[tuple(spot)].set(low).at[tuple(next_to)].set(top_value)


def shard_levels(rng, dims, pieces, least, top_value):
    def one(axis_at, shards_of):
        draws = jax.random.uniform(jax.random.fold_in(jax.random.fold_in(rng, 6), axis_at), (shards_of,), jnp.float32, least / len(pieces), top_value / len(pieces))
        return jnp.repeat(jnp.exp(draws), dims[axis_at] // shards_of).reshape((-1,) + (1,) * (len(dims) - axis_at - 1))

    loudness = one(*pieces[0])
    for cut in pieces[1:]:
        loudness = loudness * one(*cut)
    return loudness


def centred(rng, extent, width, bound, shards=(), held_as=jnp.bfloat16):
    gain = shard_levels(rng, extent, shards, -0.22, 0.18) if shards else 1.0
    entries = jax.random.normal(rng, extent, jnp.float32) * width * gain
    return jnp.minimum(jnp.maximum(entries, -bound), bound).astype(held_as)


def setup_inputs(seed: int = 0) -> dict:
    arg_keys = jax.random.split(jax.random.key(seed), 5)
    coeffs = centred(arg_keys[0], (NK, LINES, NPW, 2, NB), 0.0625, 0.5, ((0, 8), (2, 32)))
    counts = touch_ends(jax.random.randint(arg_keys[1], (NK, LINES), NPW // 2, NPW + 1), jax.random.fold_in(arg_keys[1], 1), NPW // 2, NPW).astype(jnp.int32)
    block_map = draw_block_map(jax.random.fold_in(arg_keys[4], 71), 0)
    wrap = touch_ends(jax.random.randint(arg_keys[3], (NK, LINES, NBLK), 0, BLK), jax.random.fold_in(arg_keys[3], 1), 0, BLK - 1).astype(jnp.int32)
    return dict(coeffs=coeffs, counts=counts, block_map=block_map, wrap=wrap)


def reference(coeffs, counts, block_map, wrap):
    g_ids = jnp.arange(NPW, dtype=jnp.int32)
    blk_ids = g_ids // BLK
    lane_ids = g_ids % BLK

    def margin_at(k_here):
        k_next = (k_here + 1) % NK
        per_line = []
        for line_idx in range(LINES):
            block_src = block_map[k_here, line_idx]
            wrap_src = wrap[k_here, line_idx]
            src_rows = (block_src[blk_ids] * BLK + (lane_ids + wrap_src[blk_ids]) % BLK).astype(jnp.int32)
            usable = (g_ids < counts[k_here, line_idx]) & (src_rows < counts[k_next, line_idx])
            left_side = jnp.where(usable[:, None, None], coeffs[k_here, line_idx].astype(jnp.float32), jnp.zeros((), jnp.float32))
            right_side = coeffs[k_next, line_idx][src_rows].astype(jnp.float32)
            products = jnp.einsum("gcm,gdn->mcdn", left_side, right_side, precision=lax.Precision.HIGHEST)
            real_part = products[:, 0, 0] + products[:, 1, 1]
            imag_part = products[:, 0, 1] - products[:, 1, 0]
            per_line.append(jnp.stack([real_part, imag_part], axis=1))
        return jnp.stack(per_line, axis=1)

    return lax.map(margin_at, jnp.arange(NK, dtype=jnp.int32))
```

```python
import functools

import jax
import jax.numpy as jnp
from jax import lax
from jax.experimental import pallas as pl
from jax.experimental.pallas import tpu as pltpu
from jax.sharding import PartitionSpec as P

MESH = pl.DeviceIdType.MESH
BLK = 32
ROWS = 2 * BLK
CAP = 3
NS = 32
NZ = 8
LANE = 128
NQ = 4
GRP = 4
NG = NS // GRP
STEP = CAP * ROWS
AHEAD = 4


def rem(a, b):
    return lax.rem(a, jnp.int32(b))


def div(a, b):
    return lax.div(a, jnp.int32(b))


def offset(grp, u):
    d = div(grp + 1, 2)
    edge = 1 - div(rem(grp, 7) + 6, 7)
    odd = u % 2
    dz = d * (1 - 2 * odd * (1 - edge))
    dx = ((u + 1) // 2) % 2
    dc = edge * odd + (1 - edge) * rem(grp + 1, 2)
    return dz, dx, dc


def shifted(x, z, c, off, sign):
    dz, dx, dc = off
    return rem(x + dx, 2) * 16 + rem(z + sign * dz + 16, NZ) * 2 + rem(c + dc, 2)


def kernel(send_tab, recv_tab, cin, out, send, recv, left, acc, rs1, rs2, rs3,
           ssem, rsem, s1sem, r1sem, s2sem, r2sem, s3sem, r3sem):
    k = lax.axis_index("ka")
    g = lax.axis_index("ga")
    x, z, c = div(g, 16), rem(div(g, 2), NZ), rem(g, 2)
    k_to, k_from = rem(k + 7, 8), rem(k + 1, 8)
    core_peer = x * 16 + z * 2 + (1 - c)
    x_peer = (1 - x) * 16 + z * 2 + c

    def z_peer(dz):
        return x * 16 + rem(z + dz, NZ) * 2 + c

    barrier = pltpu.get_barrier_semaphore()

    def greet(s, carry):
        pl.semaphore_signal(barrier, inc=1, device_id=(k_from, s), device_id_type=MESH)
        return carry

    lax.fori_loop(0, NS, greet, 0)
    for peer in [core_peer, x_peer] + [z_peer(dz) for dz in range(1, NZ)]:
        pl.semaphore_signal(barrier, inc=1, device_id=(k, peer), device_id_type=MESH)

    def stage(it):
        q, grp = div(it, NG), rem(it, NG)
        for u in range(GRP):
            t = shifted(x, z, c, offset(grp, u), 1)
            for r in range(CAP):
                send[q, grp * GRP + u, r * ROWS:(r + 1) * ROWS, :] = cin[q, send_tab[t * CAP + r]]

    def exchange(it, u):
        q, grp = div(it, NG), rem(it, NG)
        j = grp * GRP + u
        t = shifted(x, z, c, offset(grp, u), 1)
        return pltpu.make_async_remote_copy(
            src_ref=send.at[q, j], dst_ref=recv.at[q, j], send_sem=ssem.at[q, j], recv_sem=rsem.at[q, j],
            device_id=(k_to, t), device_id_type=MESH)

    def launch(it):
        for u in range(GRP):
            exchange(it, u).start()

    row = lax.broadcasted_iota(jnp.int32, (2 * ROWS, 4 * ROWS), 0)
    col = lax.broadcasted_iota(jnp.int32, (2 * ROWS, 4 * ROWS), 1)
    left_lane = rem(div(row, 2), BLK)
    right_lane = rem(div(col, 2), BLK)
    first = row < ROWS
    same_slot = div(row, ROWS) == rem(div(col, ROWS), 2)
    straight = col < 2 * ROWS
    same_part = rem(row, 2) == rem(col, 2)
    sign = jnp.where(straight, jnp.where(same_part, 1.0, 0.0),
                     jnp.where(same_part, 0.0, jnp.where(rem(row, 2) == 0, 1.0, -1.0)))
    pattern = jnp.where(same_slot, sign, 0.0)

    def build(grp):
        for pair in range(GRP * CAP // 2):
            slots = []
            for h in range(2):
                u, r = divmod(2 * pair + h, CAP)
                s = shifted(x, z, c, offset(grp, u), -1)
                slots.append([recv_tab[n * NS * CAP + s * CAP + r] for n in range(4)])
            (b0, w0, l0, r0), (b1, w1, l1, r1) = slots
            w = jnp.where(first, w0, w1)
            hit = left_lane == ((right_lane - w) & (BLK - 1))
            hit = hit & (left_lane < jnp.where(first, l0, l1)) & (right_lane < jnp.where(first, r0, r1))
            pick = jnp.where(hit, pattern, 0.0).astype(jnp.bfloat16)
            cols = pl.ds(pl.multiple_of(grp * (GRP * STEP) + pair * 2 * ROWS, LANE), 2 * ROWS)
            for q in range(NQ):
                held = jnp.concatenate([cin[q, b0], cin[q, b1]], axis=0)
                moved = lax.dot_general(held, pick, (((0,), (0,)), ((), ())),
                                        preferred_element_type=jnp.float32).astype(jnp.bfloat16)
                for ii in range(8):
                    i = q * 8 + ii
                    ix, iz, ic = i // 16, (i // 2) % NZ, i % 2
                    base = ((ic * 2 + ix) * NZ + iz) * 32
                    part = moved[ii * 16:(ii + 1) * 16]
                    left[base:base + 16, cols] = part[:, :LANE]
                    left[base + 16:base + 32, cols] = part[:, LANE:]

    def multiply(it):
        q, grp = div(it, NG), rem(it, NG)
        for u in range(GRP):
            exchange(it, u).wait_recv()
        j0 = grp * GRP
        cols = pl.ds(pl.multiple_of(grp * (GRP * STEP), LANE), GRP * STEP)
        right = recv[q, pl.ds(j0, GRP)].reshape(GRP * STEP, LANE)
        part = 256

        def strip(n, carry):
            rows = pl.ds(pl.multiple_of(n * part, part), part)
            val = jnp.dot(left[rows, cols], right, preferred_element_type=jnp.float32)

            @pl.when(grp == 0)
            def _():
                acc[q, rows] = val

            @pl.when(grp > 0)
            def _():
                acc[q, rows] += val

            return carry

        lax.fori_loop(0, 1024 // part, strip, 0)

    def half(which):
        return pl.ds(pl.multiple_of(which * 512, 512), 512)

    def quarter(cc, xx):
        return pl.ds(pl.multiple_of(cc * 512 + xx * 256, 256), 256)

    def piece(cc, xx, zz):
        return pl.ds(pl.multiple_of(cc * 512 + xx * 256 + zz * 32, 32), 32)

    def to_core(q):
        return pltpu.make_async_remote_copy(
            src_ref=acc.at[q, half(1 - c)], dst_ref=rs1.at[q], send_sem=s1sem.at[q], recv_sem=r1sem.at[q],
            device_id=(k, core_peer), device_id_type=MESH)

    def to_x(q):
        return pltpu.make_async_remote_copy(
            src_ref=acc.at[q, quarter(c, 1 - x)], dst_ref=rs2.at[q], send_sem=s2sem.at[q], recv_sem=r2sem.at[q],
            device_id=(k, x_peer), device_id_type=MESH)

    def to_z(q, dz):
        return pltpu.make_async_remote_copy(
            src_ref=acc.at[q, piece(c, x, rem(z + dz, NZ))], dst_ref=rs3.at[q, dz],
            send_sem=s3sem.at[q, dz], recv_sem=r3sem.at[q, dz],
            device_id=(k, z_peer(dz)), device_id_type=MESH)

    def after_core(q):
        to_core(q).wait_recv()
        acc[q, half(c)] += rs1[q]
        to_x(q).start()

    def after_x(q):
        to_x(q).wait_recv()
        acc[q, quarter(c, x)] += rs2[q]
        for dz in range(1, NZ):
            to_z(q, dz).start()

    def finish(q):
        total = acc[q, piece(c, x, z)]
        for dz in range(1, NZ):
            to_z(q, dz).wait_recv()
            total = total + rs3[q, dz]
        out[0, :, q * LANE:(q + 1) * LANE] = total[:16]
        out[1, :, q * LANE:(q + 1) * LANE] = total[16:]

    stage(jnp.int32(0))
    pl.semaphore_wait(barrier, NS + 2 + NZ - 1)

    def start(it, carry):
        launch(it)
        stage(it + 1)
        return carry

    lax.fori_loop(0, AHEAD, start, 0)
    total_its = NQ * NG

    def body(it, carry):
        q, grp = div(it, NG), rem(it, NG)

        @pl.when(it + AHEAD < total_its)
        def _():
            launch(it + AHEAD)

        @pl.when(it + AHEAD + 1 < total_its)
        def _():
            stage(it + AHEAD + 1)

        @pl.when(q == 0)
        def _():
            build(grp)

        @pl.when((q > 0) & (grp == 0))
        def _():
            to_core(q - 1).start()

        @pl.when((q > 0) & (grp == 2))
        def _():
            after_core(q - 1)

        @pl.when((q > 0) & (grp == 4))
        def _():
            after_x(q - 1)

        multiply(it)
        return carry

    lax.fori_loop(0, total_its, body, 0)
    last = NQ - 1
    to_core(last).start()
    after_core(last)
    after_x(last)
    for q in range(NQ):
        finish(q)

    def drain(it, carry):
        for u in range(GRP):
            exchange(it, u).wait_send()
        return carry

    lax.fori_loop(0, total_its, drain, 0)
    for q in range(NQ):
        to_core(q).wait_send()
        to_x(q).wait_send()
        for dz in range(1, NZ):
            to_z(q, dz).wait_send()


def slots(hit, values):
    depth = hit.shape[-1]
    tri = (jnp.arange(depth)[:, None] <= jnp.arange(depth)[None, :]).astype(jnp.bfloat16)
    place = jnp.dot(hit.astype(jnp.bfloat16), tri, preferred_element_type=jnp.float32).astype(jnp.int32) - 1
    chosen = hit[:, None, :] & (place[:, None, :] == jnp.arange(CAP)[None, :, None])
    return [jnp.sum(jnp.where(chosen, v, 0), axis=-1).reshape(-1) for v in values]


def local(coeffs, counts, block_map, wrap):
    k = lax.axis_index("ka")
    g = lax.axis_index("ga")
    per = block_map.shape[-1] // NS
    shard = jnp.arange(NS, dtype=jnp.int32)
    to_map = block_map[(k + 7) % 8, 0].reshape(NS, per)
    (send_tab,) = slots(to_map // per == g, [to_map[:, None, :] % per])
    mine = lax.dynamic_slice_in_dim(block_map[k, 0], g * per, per)
    turn = lax.dynamic_slice_in_dim(wrap[k, 0], g * per, per)
    ids = jnp.arange(per, dtype=jnp.int32)
    left_lim = counts[k, 0] - (g * per + ids) * BLK
    right_lim = counts[(k + 1) % 8, 0] - mine * BLK
    recv_tab = jnp.concatenate(slots(mine[None, :] // per == shard[:, None], [ids, turn, left_lim, right_lim]))
    cin = coeffs.reshape(per, BLK, 2, NQ, LANE).transpose(3, 0, 1, 2, 4).reshape(NQ, per, ROWS, LANE)
    vmem = pl.BlockSpec(memory_space=pltpu.VMEM)
    smem = pl.BlockSpec(memory_space=pltpu.SMEM)
    dma = pltpu.SemaphoreType.DMA
    out = pl.pallas_call(
        kernel,
        out_shape=jax.ShapeDtypeStruct((2, 16, NQ * LANE), jnp.float32),
        in_specs=[smem, smem, vmem],
        out_specs=vmem,
        scratch_shapes=[
            pltpu.VMEM((NQ, NS, STEP, LANE), jnp.bfloat16),
            pltpu.VMEM((NQ, NS, STEP, LANE), jnp.bfloat16),
            pltpu.VMEM((1024, NS * STEP), jnp.bfloat16),
            pltpu.VMEM((NQ, 1024, LANE), jnp.float32),
            pltpu.VMEM((NQ, 512, LANE), jnp.float32),
            pltpu.VMEM((NQ, 256, LANE), jnp.float32),
            pltpu.VMEM((NQ, NZ, 32, LANE), jnp.float32),
            dma((NQ, NS)), dma((NQ, NS)), dma((NQ,)), dma((NQ,)), dma((NQ,)), dma((NQ,)),
            dma((NQ, NZ)), dma((NQ, NZ)),
        ],
        compiler_params=pltpu.CompilerParams(
            collective_id=0, has_side_effects=True, vmem_limit_bytes=48 << 20),
    )(send_tab, recv_tab, cin)
    return out.transpose(1, 0, 2)[None, :, None]


def solution(mesh):
    placed = (P("ka", None, "ga", None, None), P(), P(), P())
    return jax.shard_map(
        local,
        mesh=mesh,
        in_specs=placed,
        out_specs=P("ka", "ga", None, None, None),
        check_vma=False,
    )
```

```python
import functools

import jax
import jax.numpy as jnp
from jax import lax
from jax.experimental import pallas as pl
from jax.experimental.pallas import tpu as pltpu
from jax.sharding import PartitionSpec as P

MESH = pl.DeviceIdType.MESH
BLK = 32
ROWS = 2 * BLK
CAP = 3
NS = 32
NZ = 8
LANE = 128
NQ = 4
GRP = 4
NG = NS // GRP
STEP = CAP * ROWS
AHEAD = 4
RELAYED = (1, 2)
DIRECT = (0, 3)
NR = len(RELAYED)


def rem(a, b):
    return lax.rem(a, jnp.int32(b))


def div(a, b):
    return lax.div(a, jnp.int32(b))


def offset(grp, u):
    grp = NG - 1 - grp
    d = div(grp + 1, 2)
    edge = 1 - div(rem(grp, 7) + 6, 7)
    odd = u % 2
    dz = d * (1 - 2 * odd * (1 - edge))
    dx = ((u + 1) // 2) % 2
    dc = edge * odd + (1 - edge) * rem(grp + 1, 2)
    return dz, dx, dc


def shifted(x, z, c, off, sign):
    dz, dx, dc = off
    return rem(x + dx, 2) * 16 + rem(z + sign * dz + 16, NZ) * 2 + rem(c + dc, 2)


def prepare(counts, block_map, wrap, coeffs, cin, send_tab, recv_tab, sem):
    copies = [pltpu.make_async_copy(coeffs.at[:, :, pl.ds(q * LANE, LANE)], cin.at[q], sem.at[q]) for q in range(NQ)]
    for copy in copies:
        copy.start()
    k = lax.axis_index("ka")
    g = lax.axis_index("ga")
    k_to, k_from = rem(k + 7, 8), rem(k + 1, 8)

    def shape_iota(rows, dim):
        return lax.broadcasted_iota(jnp.int32, (rows, LANE), dim)

    tri = (shape_iota(LANE, 0) <= shape_iota(LANE, 1)) & (div(shape_iota(LANE, 0), 64) == div(shape_iota(LANE, 1), 64))
    tri = jnp.where(tri, 1.0, 0.0).astype(jnp.bfloat16)

    def place(hit):
        return jnp.dot(jnp.where(hit, 1.0, 0.0).astype(jnp.bfloat16), tri, preferred_element_type=jnp.float32)

    def table(rows, columns):
        lane = shape_iota(rows, 1)
        held = jnp.zeros((rows, LANE), jnp.float32)
        for n, (mask, value) in enumerate(columns):
            held = jnp.where(lane == n, jnp.sum(jnp.where(mask, value, 0.0), axis=1, keepdims=True), held)
        return held.astype(jnp.int32)

    to_map = block_map[pl.ds(k_to * 16, 16), :]
    hit = (to_map >> 6) == g
    rank = place(hit)
    half = shape_iota(16, 1) >> 6
    value = (to_map & 63).astype(jnp.float32)
    send_tab[...] = table(16, [(hit & (rank == r + 1.0) & (half == h), value) for h in range(2) for r in range(CAP)])

    at = pl.ds(k * 16 + div(g, 2), 1)
    mine = block_map[at, :]
    ids = shape_iota(1, 1) & 63
    left_lim = counts[k, 0] - (g * 64 + ids) * BLK
    right_lim = counts[k_from, 0] - mine * BLK
    hit = (shape_iota(NS, 0) == (mine >> 6)) & ((shape_iota(NS, 1) >> 6) == rem(g, 2))
    rank = place(hit)
    recv_tab[...] = table(NS, [(hit & (rank == r + 1.0), v.astype(jnp.float32))
                               for v in (ids, wrap[at, :], left_lim, right_lim) for r in range(CAP)])
    for copy in copies:
        copy.wait()


def kernel(send_tab, recv_tab, cin, out, send, recv, relay, left, acc, rs1, rs2, rs3,
           ssem, rsem, lsem, fsem, s1sem, r1sem, s2sem, r2sem, s3sem, r3sem):
    k = lax.axis_index("ka")
    g = lax.axis_index("ga")
    x, z, c = div(g, 16), rem(div(g, 2), NZ), rem(g, 2)
    k_to, k_from = rem(k + 7, 8), rem(k + 1, 8)
    core_peer = x * 16 + z * 2 + (1 - c)
    x_peer = (1 - x) * 16 + z * 2 + c

    def z_peer(dz):
        return x * 16 + rem(z + dz, NZ) * 2 + c

    barrier = pltpu.get_barrier_semaphore()

    even = rem(k, 2) == 0
    k_relay = rem(k + 6, 8)
    flipped = (1 - x) * 16 + z * 2 + c

    def greet(kk, steps):
        def one(grp, carry):
            for u in steps:
                s = shifted(x, z, c, offset(grp, u), -1)
                pl.semaphore_signal(barrier, inc=1, device_id=(kk, s), device_id_type=MESH)
            return carry

        lax.fori_loop(0, NG, one, 0)

    greet(k_from, DIRECT)

    @pl.when(even)
    def _():
        greet(k_from, RELAYED)

        def one(grp, carry):
            for u in RELAYED:
                s = x * 16 + rem(shifted(x, z, c, offset(grp, u), -1), 16)
                pl.semaphore_signal(barrier, inc=1, device_id=(rem(k + 2, 8), s), device_id_type=MESH)
            return carry

        lax.fori_loop(0, NG, one, 0)

    @pl.when(rem(k, 2) == 1)
    def _():
        pl.semaphore_signal(barrier, inc=1, device_id=(k_to, flipped), device_id_type=MESH)

    for peer in [core_peer, x_peer] + [z_peer(dz) for dz in range(1, NZ)]:
        pl.semaphore_signal(barrier, inc=1, device_id=(k, peer), device_id_type=MESH)

    def stage(it):
        q, grp = div(it, NG), rem(it, NG)
        for u in range(GRP):
            t = shifted(x, z, c, offset(grp, u), 1)
            for r in range(CAP):
                send[q, grp * GRP + u, r * ROWS:(r + 1) * ROWS, :] = cin[q, send_tab[div(t, 2), rem(t, 2) * CAP + r]]

    def exchange(it, u):
        q, grp = div(it, NG), rem(it, NG)
        j = grp * GRP + u
        t = shifted(x, z, c, offset(grp, u), 1)
        return pltpu.make_async_remote_copy(
            src_ref=send.at[q, j], dst_ref=recv.at[q, j], send_sem=ssem.at[q, j], recv_sem=rsem.at[q, j],
            device_id=(k_to, t), device_id_type=MESH)

    def to_relay(it, n):
        q, grp = div(it, NG), rem(it, NG)
        t = x * 16 + rem(shifted(x, z, c, offset(grp, RELAYED[n]), 1), 16)
        return pltpu.make_async_remote_copy(
            src_ref=send.at[q, grp * GRP + RELAYED[n]], dst_ref=relay.at[q, grp * NR + n],
            send_sem=ssem.at[q, grp * GRP + RELAYED[n]], recv_sem=lsem.at[q, grp * NR + n],
            device_id=(k_relay, t), device_id_type=MESH)

    def forward(it, n):
        q, grp = div(it, NG), rem(it, NG)
        j = grp * GRP + RELAYED[n]
        return pltpu.make_async_remote_copy(
            src_ref=relay.at[q, grp * NR + n], dst_ref=recv.at[q, j],
            send_sem=fsem.at[q, grp * NR + n], recv_sem=rsem.at[q, j],
            device_id=(k_from, flipped), device_id_type=MESH)

    def launch(it):
        @pl.when(even)
        def _():
            for n in range(NR):
                to_relay(it, n).start()

        @pl.when(rem(k, 2) == 1)
        def _():
            for u in RELAYED:
                exchange(it, u).start()

        for u in DIRECT:
            exchange(it, u).start()

    def pass_on(it):
        @pl.when(even)
        def _():
            for n in range(NR):
                to_relay(it, n).wait_recv()
                forward(it, n).start()

    row = lax.broadcasted_iota(jnp.int32, (2 * ROWS, 4 * ROWS), 0)
    col = lax.broadcasted_iota(jnp.int32, (2 * ROWS, 4 * ROWS), 1)
    left_lane = rem(div(row, 2), BLK)
    right_lane = rem(div(col, 2), BLK)
    first = row < ROWS
    same_slot = div(row, ROWS) == rem(div(col, ROWS), 2)
    straight = col < 2 * ROWS
    same_part = rem(row, 2) == rem(col, 2)
    sign = jnp.where(straight, jnp.where(same_part, 1.0, 0.0),
                     jnp.where(same_part, 0.0, jnp.where(rem(row, 2) == 0, 1.0, -1.0)))
    pattern = jnp.where(same_slot, sign, 0.0)

    def build(grp):
        for pair in range(GRP * CAP // 2):
            slots = []
            for h in range(2):
                u, r = divmod(2 * pair + h, CAP)
                s = shifted(x, z, c, offset(grp, u), -1)
                slots.append([recv_tab[s, n * CAP + r] for n in range(4)])
            (b0, w0, l0, r0), (b1, w1, l1, r1) = slots
            w = jnp.where(first, w0, w1)
            hit = left_lane == ((right_lane - w) & (BLK - 1))
            hit = hit & (left_lane < jnp.where(first, l0, l1)) & (right_lane < jnp.where(first, r0, r1))
            pick = jnp.where(hit, pattern, 0.0).astype(jnp.bfloat16)
            cols = pl.ds(pl.multiple_of(grp * (GRP * STEP) + pair * 2 * ROWS, LANE), 2 * ROWS)
            for q in range(NQ):
                held = jnp.concatenate([cin[q, b0], cin[q, b1]], axis=0)
                moved = lax.dot_general(held, pick, (((0,), (0,)), ((), ())),
                                        preferred_element_type=jnp.float32).astype(jnp.bfloat16)
                for ii in range(8):
                    i = q * 8 + ii
                    ix, iz, ic = i // 16, (i // 2) % NZ, i % 2
                    base = ((ic * 2 + ix) * NZ + iz) * 32
                    part = moved[ii * 16:(ii + 1) * 16]
                    left[base:base + 16, cols] = part[:, :LANE]
                    left[base + 16:base + 32, cols] = part[:, LANE:]

    def multiply(it):
        q, grp = div(it, NG), rem(it, NG)
        for u in range(GRP):
            exchange(it, u).wait_recv()
        j0 = grp * GRP
        cols = pl.ds(pl.multiple_of(grp * (GRP * STEP), LANE), GRP * STEP)
        right = recv[q, pl.ds(j0, GRP)].reshape(GRP * STEP, LANE)
        part = 256

        def strip(n, carry):
            rows = pl.ds(pl.multiple_of(n * part, part), part)
            val = jnp.dot(left[rows, cols], right, preferred_element_type=jnp.float32)

            @pl.when(grp == 0)
            def _():
                acc[q, rows] = val

            @pl.when(grp > 0)
            def _():
                acc[q, rows] += val

            return carry

        lax.fori_loop(0, 1024 // part, strip, 0)

    def half(which):
        return pl.ds(pl.multiple_of(which * 512, 512), 512)

    def quarter(cc, xx):
        return pl.ds(pl.multiple_of(cc * 512 + xx * 256, 256), 256)

    def piece(cc, xx, zz):
        return pl.ds(pl.multiple_of(cc * 512 + xx * 256 + zz * 32, 32), 32)

    def to_core(q):
        return pltpu.make_async_remote_copy(
            src_ref=acc.at[q, half(1 - c)], dst_ref=rs1.at[q], send_sem=s1sem.at[q], recv_sem=r1sem.at[q],
            device_id=(k, core_peer), device_id_type=MESH)

    def to_x(q):
        return pltpu.make_async_remote_copy(
            src_ref=acc.at[q, quarter(c, 1 - x)], dst_ref=rs2.at[q], send_sem=s2sem.at[q], recv_sem=r2sem.at[q],
            device_id=(k, x_peer), device_id_type=MESH)

    def to_z(q, dz):
        return pltpu.make_async_remote_copy(
            src_ref=acc.at[q, piece(c, x, rem(z + dz, NZ))], dst_ref=rs3.at[q, dz],
            send_sem=s3sem.at[q, dz], recv_sem=r3sem.at[q, dz],
            device_id=(k, z_peer(dz)), device_id_type=MESH)

    def after_core(q):
        to_core(q).wait_recv()
        acc[q, half(c)] += rs1[q]
        to_x(q).start()

    def after_x(q):
        to_x(q).wait_recv()
        acc[q, quarter(c, x)] += rs2[q]
        for dz in range(1, NZ):
            to_z(q, dz).start()

    def finish(q):
        total = acc[q, piece(c, x, z)]
        for dz in range(1, NZ):
            to_z(q, dz).wait_recv()
            total = total + rs3[q, dz]
        out[0, :, q * LANE:(q + 1) * LANE] = total[:16]
        out[1, :, q * LANE:(q + 1) * LANE] = total[16:]

    stage(jnp.int32(0))
    pl.semaphore_wait(barrier, NS + 2 + NZ - 1 + (1 - rem(k, 2)))

    def start(it, carry):
        launch(it)
        stage(it + 1)
        return carry

    lax.fori_loop(0, AHEAD, start, 0)
    total_its = NQ * NG

    def body(it, carry):
        q, grp = div(it, NG), rem(it, NG)

        @pl.when(it + AHEAD < total_its)
        def _():
            launch(it + AHEAD)

        @pl.when(it + AHEAD + 1 < total_its)
        def _():
            stage(it + AHEAD + 1)

        @pl.when(q == 0)
        def _():
            build(grp)

        @pl.when((q > 0) & (grp == 0))
        def _():
            to_core(q - 1).start()

        @pl.when((q > 0) & (grp == 2))
        def _():
            after_core(q - 1)

        @pl.when((q > 0) & (grp == 4))
        def _():
            after_x(q - 1)

        pass_on(it)
        multiply(it)
        return carry

    lax.fori_loop(0, total_its, body, 0)
    last = NQ - 1
    to_core(last).start()
    after_core(last)
    after_x(last)
    for q in range(NQ):
        finish(q)

    def drain(it, carry):
        for u in range(GRP):
            exchange(it, u).wait_send()

        @pl.when(even)
        def _():
            for n in range(NR):
                forward(it, n).wait_send()

        return carry

    lax.fori_loop(0, total_its, drain, 0)
    for q in range(NQ):
        to_core(q).wait_send()
        to_x(q).wait_send()
        for dz in range(1, NZ):
            to_z(q, dz).wait_send()


def local(coeffs, counts, block_map, wrap):
    _, _, rows, parts, bands = coeffs.shape
    vmem = pl.BlockSpec(memory_space=pltpu.VMEM)
    smem = pl.BlockSpec(memory_space=pltpu.SMEM)
    dma = pltpu.SemaphoreType.DMA
    cin, send_tab, recv_tab = pl.pallas_call(
        prepare,
        out_shape=[
            jax.ShapeDtypeStruct((NQ, rows, parts, LANE), coeffs.dtype),
            jax.ShapeDtypeStruct((16, LANE), jnp.int32),
            jax.ShapeDtypeStruct((NS, LANE), jnp.int32),
        ],
        in_specs=[smem, vmem, vmem, pl.BlockSpec(memory_space=pltpu.HBM)],
        out_specs=[vmem, vmem, vmem],
        scratch_shapes=[dma((NQ,))],
        compiler_params=pltpu.CompilerParams(vmem_limit_bytes=8 << 20),
    )(counts, block_map.reshape(-1, LANE), wrap.reshape(-1, LANE), coeffs.reshape(rows, parts, bands))
    cin = cin.reshape(NQ, rows // BLK, ROWS, LANE)
    out = pl.pallas_call(
        kernel,
        out_shape=jax.ShapeDtypeStruct((2, 16, NQ * LANE), jnp.float32),
        in_specs=[smem, smem, vmem],
        out_specs=vmem,
        scratch_shapes=[
            pltpu.VMEM((NQ, NS, STEP, LANE), jnp.bfloat16),
            pltpu.VMEM((NQ, NS, STEP, LANE), jnp.bfloat16),
            pltpu.VMEM((NQ, NG * NR, STEP, LANE), jnp.bfloat16),
            pltpu.VMEM((1024, NS * STEP), jnp.bfloat16),
            pltpu.VMEM((NQ, 1024, LANE), jnp.float32),
            pltpu.VMEM((NQ, 512, LANE), jnp.float32),
            pltpu.VMEM((NQ, 256, LANE), jnp.float32),
            pltpu.VMEM((NQ, NZ, 32, LANE), jnp.float32),
            dma((NQ, NS)), dma((NQ, NS)), dma((NQ, NG * NR)), dma((NQ, NG * NR)),
            dma((NQ,)), dma((NQ,)), dma((NQ,)), dma((NQ,)),
            dma((NQ, NZ)), dma((NQ, NZ)),
        ],
        compiler_params=pltpu.CompilerParams(
            collective_id=0, has_side_effects=True, vmem_limit_bytes=48 << 20),
    )(send_tab, recv_tab, cin)
    return out.transpose(1, 0, 2)[None, :, None]


def solution(mesh):
    placed = (P("ka", None, "ga", None, None), P(), P(), P())
    return jax.shard_map(
        local,
        mesh=mesh,
        in_specs=placed,
        out_specs=P("ka", "ga", None, None, None),
        check_vma=False,
    )
```

```python
import functools

import jax
import jax.numpy as jnp
from jax import lax
from jax.experimental import pallas as pl
from jax.experimental.pallas import tpu as pltpu
from jax.sharding import PartitionSpec as P

MESH = pl.DeviceIdType.MESH
BLK = 32
ROWS = 2 * BLK
CAP = 3
NS = 32
NZ = 8
NX = 2
LANE = 128
NQ = 4
GRP = 4
NG = NS // GRP
STEP = CAP * ROWS
AHEAD = 20
RELAYED = (1, 2)
DIRECT = (0, 3)
NR = len(RELAYED)
TOTAL = NQ * NG
RELAY_END = TOTAL - 3


def rem(a, b):
    return lax.rem(a, jnp.int32(b))


def div(a, b):
    return lax.div(a, jnp.int32(b))


def offset(grp, u):
    grp = NG - 1 - grp
    d = div(grp + 1, 2)
    edge = 1 - div(rem(grp, 7) + 6, 7)
    odd = u % 2
    dz = d * (1 - 2 * odd * (1 - edge))
    dx = ((u + 1) // 2) % 2
    dc = edge * odd + (1 - edge) * rem(grp + 1, 2)
    return dz, dx, dc


def shifted(x, z, c, off, sign):
    dz, dx, dc = off
    return rem(x + dx, 2) * 16 + rem(z + sign * dz + 16, NZ) * 2 + rem(c + dc, 2)


def iota(rows, dim):
    return lax.broadcasted_iota(jnp.int32, (rows, LANE), dim)


def make_tables(k, g, counts, maps, send_tab, recv_tab):
    def place(hit):
        lane = iota(hit.shape[0], 1) & 63
        count = jnp.where(hit, 1, 0)
        for shift in (1, 2, 4, 8, 16, 32):
            count = count + jnp.where(lane >= shift, pltpu.roll(count, shift, 1), 0)
        return count

    def table(rows, columns):
        lane = iota(rows, 1)
        held = jnp.zeros((rows, LANE), jnp.int32)
        for n, (mask, value) in enumerate(columns):
            held = jnp.where(lane == n, jnp.sum(jnp.where(mask, value, 0), axis=1, keepdims=True), held)
        return held

    to_map = maps[0]
    hit = (to_map >> 6) == g
    rank = place(hit)
    half = iota(16, 1) >> 6
    value = to_map & 63
    send_tab[...] = table(16, [(hit & (rank == r + 1) & (half == h), value) for h in range(2) for r in range(CAP)])

    at = pl.ds(div(g, 2), 1)
    mine = maps[1, at, :]
    ids = iota(1, 1) & 63
    left_lim = counts[k] - (g * 64 + ids) * BLK
    right_lim = counts[rem(k + 1, 8)] - mine * BLK
    hit = (iota(NS, 0) == (mine >> 6)) & ((iota(NS, 1) >> 6) == rem(g, 2))
    rank = place(hit)
    recv_tab[...] = table(NS, [(hit & (rank == r + 1), v)
                               for v in (ids, maps[2, at, :], left_lim, right_lim) for r in range(CAP)])


def kernel(counts, block_map, wrap, coeffs, out, cin, maps, send_vec, recv_vec, send_tab, recv_tab,
           send, recv, relay, left, flat, acc, rs1, rs2, rs3, rs4, csem, map_sem, tab_sem,
           ssem, rsem, lsem, fsem, s1sem, r1sem, s2sem, r2sem, s3sem, r3sem, s4sem, r4sem):
    k = lax.axis_index("ka")
    g = lax.axis_index("ga")
    x, z, c = div(g, 16), rem(div(g, 2), NZ), rem(g, 2)
    k_to, k_from = rem(k + 7, 8), rem(k + 1, 8)
    core_peer = x * 16 + z * 2 + (1 - c)
    x_peer = (1 - x) * 16 + z * 2 + c

    def any_peer(dx, dz):
        return rem(x + dx, NX) * 16 + rem(z + dz, NZ) * 2 + c

    def map_rows(kk):
        return pl.ds(pl.multiple_of(kk * 16, 16), 16)

    fetches = [pltpu.make_async_copy(source.at[map_rows(kk)], maps.at[n], map_sem.at[n])
               for n, (source, kk) in enumerate(((block_map, k_to), (block_map, k), (wrap, k)))]
    copies = [pltpu.make_async_copy(coeffs.at[:, :, pl.ds(q * LANE, LANE)], cin.at[q], csem.at[q]) for q in range(NQ)]
    for copy in fetches + copies:
        copy.start()

    barrier = pltpu.get_barrier_semaphore()

    even = rem(k, 2) == 0
    k_relay = rem(k + 6, 8)
    flipped = (1 - x) * 16 + z * 2 + c

    def greet(kk, steps):
        def one(grp, carry):
            for u in steps:
                s = shifted(x, z, c, offset(grp, u), -1)
                pl.semaphore_signal(barrier, inc=1, device_id=(kk, s), device_id_type=MESH)
            return carry

        lax.fori_loop(0, NG, one, 0)

    greet(k_from, range(GRP))

    @pl.when(even)
    def _():
        def one(grp, carry):
            for u in RELAYED:
                s = x * 16 + rem(shifted(x, z, c, offset(grp, u), -1), 16)
                pl.semaphore_signal(barrier, inc=1, device_id=(rem(k + 2, 8), s), device_id_type=MESH)
            return carry

        lax.fori_loop(0, NG, one, 0)

    @pl.when(rem(k, 2) == 1)
    def _():
        pl.semaphore_signal(barrier, inc=1, device_id=(k_to, flipped), device_id_type=MESH)

    for peer in [core_peer] + [any_peer(dx, dz) for dx in range(NX) for dz in range(NZ) if dx or dz]:
        pl.semaphore_signal(barrier, inc=1, device_id=(k, peer), device_id_type=MESH)

    def stage(it):
        q, grp = div(it, NG), rem(it, NG)
        for u in range(GRP):
            t = shifted(x, z, c, offset(grp, u), 1)
            for r in range(CAP):
                blk = send_tab[div(t, 2), rem(t, 2) * CAP + r] & 63
                send[q, grp * GRP + u, r * BLK:(r + 1) * BLK] = cin[q, pl.ds(blk * BLK, BLK)]

    def exchange(it, u):
        q, grp = div(it, NG), rem(it, NG)
        j = grp * GRP + u
        t = shifted(x, z, c, offset(grp, u), 1)
        return pltpu.make_async_remote_copy(
            src_ref=send.at[q, j], dst_ref=recv.at[q, j], send_sem=ssem.at[q, j], recv_sem=rsem.at[q, j],
            device_id=(k_to, t), device_id_type=MESH)

    def to_relay(it, n):
        q, grp = div(it, NG), rem(it, NG)
        t = x * 16 + rem(shifted(x, z, c, offset(grp, RELAYED[n]), 1), 16)
        return pltpu.make_async_remote_copy(
            src_ref=send.at[q, grp * GRP + RELAYED[n]], dst_ref=relay.at[q, grp * NR + n],
            send_sem=ssem.at[q, grp * GRP + RELAYED[n]], recv_sem=lsem.at[q, grp * NR + n],
            device_id=(k_relay, t), device_id_type=MESH)

    def forward(it, n):
        q, grp = div(it, NG), rem(it, NG)
        j = grp * GRP + RELAYED[n]
        return pltpu.make_async_remote_copy(
            src_ref=relay.at[q, grp * NR + n], dst_ref=recv.at[q, j],
            send_sem=fsem.at[q, grp * NR + n], recv_sem=rsem.at[q, j],
            device_id=(k_from, flipped), device_id_type=MESH)

    def launch(it):
        @pl.when(even & (it < RELAY_END))
        def _():
            for n in range(NR):
                to_relay(it, n).start()

        @pl.when(jnp.logical_not(even & (it < RELAY_END)))
        def _():
            for u in RELAYED:
                exchange(it, u).start()

        for u in DIRECT:
            exchange(it, u).start()

    def pass_on(it):
        @pl.when(even & (it < RELAY_END))
        def _():
            for n in range(NR):
                to_relay(it, n).wait_recv()
                forward(it, n).start()

    row = lax.broadcasted_iota(jnp.int32, (2 * ROWS, 4 * ROWS), 0)
    col = lax.broadcasted_iota(jnp.int32, (2 * ROWS, 4 * ROWS), 1)
    left_lane = rem(div(row, 2), BLK)
    right_lane = rem(div(col, 2), BLK)
    first = row < ROWS
    same_slot = div(row, ROWS) == rem(div(col, ROWS), 2)
    straight = col < 2 * ROWS
    same_part = rem(row, 2) == rem(col, 2)
    sign = jnp.where(straight, jnp.where(same_part, 1.0, 0.0),
                     jnp.where(same_part, 0.0, jnp.where(rem(row, 2) == 0, 1.0, -1.0)))
    pattern = jnp.where(same_slot, sign, 0.0)

    def build(grp):
        for pair in range(GRP * CAP // 2):
            slots = []
            for h in range(2):
                u, r = divmod(2 * pair + h, CAP)
                s = shifted(x, z, c, offset(grp, u), -1)
                slots.append([recv_tab[s, n * CAP + r] for n in range(4)])
            (b0, w0, l0, r0), (b1, w1, l1, r1) = slots
            w = jnp.where(first, w0, w1)
            hit = left_lane == ((right_lane - w) & (BLK - 1))
            hit = hit & (left_lane < jnp.where(first, l0, l1)) & (right_lane < jnp.where(first, r0, r1))
            pick = jnp.where(hit, pattern, 0.0).astype(jnp.bfloat16)
            cols = pl.ds(pl.multiple_of(grp * (GRP * STEP) + pair * 2 * ROWS, LANE), 2 * ROWS)
            for q in range(NQ):
                held = jnp.concatenate([cin[q, pl.ds((b & 63) * BLK, BLK)].reshape(ROWS, LANE) for b in (b0, b1)], axis=0)
                moved = lax.dot_general(held, pick, (((0,), (0,)), ((), ())),
                                        preferred_element_type=jnp.float32).astype(jnp.bfloat16)
                for ii in range(8):
                    i = q * 8 + ii
                    ix, iz, ic = i // 16, (i // 2) % NZ, i % 2
                    base = ((ic * 2 + ix) * NZ + iz) * 32
                    part = moved[ii * 16:(ii + 1) * 16]
                    left[base:base + 16, cols] = part[:, :LANE]
                    left[base + 16:base + 32, cols] = part[:, LANE:]

    def multiply(it):
        q, grp = div(it, NG), rem(it, NG)
        for u in range(GRP):
            exchange(it, u).wait_recv()
        j0 = grp * GRP
        cols = pl.ds(pl.multiple_of(grp * (GRP * STEP), LANE), GRP * STEP)
        for u in range(GRP):
            flat[u * STEP:(u + 1) * STEP] = recv[q, j0 + u].reshape(STEP, LANE)
        part = 256

        def strip(n, carry):
            rows = pl.ds(pl.multiple_of(n * part, part), part)
            val = jnp.dot(left[rows, cols], flat[...], preferred_element_type=jnp.float32)

            @pl.when(grp == 0)
            def _():
                acc[q, rows] = val

            @pl.when(grp > 0)
            def _():
                acc[q, rows] += val

            return carry

        lax.fori_loop(0, 1024 // part, strip, 0)

    def half(which):
        return pl.ds(pl.multiple_of(which * 512, 512), 512)

    def quarter(cc, xx):
        return pl.ds(pl.multiple_of(cc * 512 + xx * 256, 256), 256)

    def piece(cc, xx, zz):
        return pl.ds(pl.multiple_of(cc * 512 + xx * 256 + zz * 32, 32), 32)

    def to_core(q):
        return pltpu.make_async_remote_copy(
            src_ref=acc.at[q, half(1 - c)], dst_ref=rs1.at[q], send_sem=s1sem.at[q], recv_sem=r1sem.at[q],
            device_id=(k, core_peer), device_id_type=MESH)

    def to_x(q):
        return pltpu.make_async_remote_copy(
            src_ref=acc.at[q, quarter(c, 1 - x)], dst_ref=rs2.at[q], send_sem=s2sem.at[q], recv_sem=r2sem.at[q],
            device_id=(k, x_peer), device_id_type=MESH)

    def to_z(q, dz):
        return pltpu.make_async_remote_copy(
            src_ref=acc.at[q, piece(c, x, rem(z + dz, NZ))], dst_ref=rs3.at[q, dz],
            send_sem=s3sem.at[q, dz], recv_sem=r3sem.at[q, dz],
            device_id=(k, any_peer(0, dz)), device_id_type=MESH)

    def to_any(q, dx, dz):
        n = dx * NZ + dz
        return pltpu.make_async_remote_copy(
            src_ref=acc.at[q, piece(c, rem(x + dx, NX), rem(z + dz, NZ))], dst_ref=rs4.at[n],
            send_sem=s4sem.at[n], recv_sem=r4sem.at[n],
            device_id=(k, any_peer(dx, dz)), device_id_type=MESH)

    def after_core(q):
        to_core(q).wait_recv()
        acc[q, half(c)] += rs1[q]
        to_x(q).start()

    def after_x(q):
        to_x(q).wait_recv()
        acc[q, quarter(c, x)] += rs2[q]
        for dz in range(1, NZ):
            to_z(q, dz).start()

    def finish(q):
        total = acc[q, piece(c, x, z)]
        for dz in range(1, NZ):
            to_z(q, dz).wait_recv()
            total = total + rs3[q, dz]
        out[0, :, q * LANE:(q + 1) * LANE] = total[:16]
        out[1, :, q * LANE:(q + 1) * LANE] = total[16:]

    far_first = sorted(((dx, dz) for dx in range(NX) for dz in range(NZ) if dx or dz),
                       key=lambda p: -min(p[1], NZ - p[1]))

    def spread(q):
        to_core(q).wait_recv()
        acc[q, half(c)] += rs1[q]
        for dx, dz in far_first:
            to_any(q, dx, dz).start()

    def finish_last(q):
        total = acc[q, piece(c, x, z)]
        for dx, dz in reversed(far_first):
            to_any(q, dx, dz).wait_recv()
            total = total + rs4[dx * NZ + dz]
        out[0, :, q * LANE:(q + 1) * LANE] = total[:16]
        out[1, :, q * LANE:(q + 1) * LANE] = total[16:]

    for copy in fetches:
        copy.wait()
    make_tables(k, g, counts, maps, send_vec, recv_vec)
    tables = [pltpu.make_async_copy(vec, tab, tab_sem.at[n])
              for n, (vec, tab) in enumerate(((send_vec, send_tab), (recv_vec, recv_tab)))]
    for copy in tables:
        copy.start()
    for copy in tables + copies:
        copy.wait()
    stage(jnp.int32(0))
    pl.semaphore_wait(barrier, NS + NX * NZ + (1 - rem(k, 2)) * 17)

    def start(it, carry):
        launch(it)
        stage(it + 1)
        return carry

    lax.fori_loop(0, AHEAD, start, 0)

    def body(it, carry):
        q, grp = div(it, NG), rem(it, NG)

        @pl.when(it + AHEAD < TOTAL)
        def _():
            launch(it + AHEAD)

        @pl.when(it + AHEAD + 1 < TOTAL)
        def _():
            stage(it + AHEAD + 1)

        @pl.when(q == 0)
        def _():
            build(grp)

        @pl.when((q > 0) & (grp == 0))
        def _():
            to_core(q - 1).start()

        @pl.when((q > 0) & (grp == 2))
        def _():
            after_core(q - 1)

        @pl.when((q > 0) & (grp == 4))
        def _():
            after_x(q - 1)

        pass_on(it)
        multiply(it)
        return carry

    lax.fori_loop(0, TOTAL, body, 0)
    last = NQ - 1
    to_core(last).start()
    spread(last)
    for q in range(last):
        finish(q)
    finish_last(last)

    def drain(it, carry):
        for u in range(GRP):
            exchange(it, u).wait_send()

        @pl.when(even & (it < RELAY_END))
        def _():
            for n in range(NR):
                forward(it, n).wait_send()

        return carry

    lax.fori_loop(0, TOTAL, drain, 0)
    for q in range(NQ):
        to_core(q).wait_send()
    for q in range(last):
        to_x(q).wait_send()
        for dz in range(1, NZ):
            to_z(q, dz).wait_send()
    for dx, dz in far_first:
        to_any(last, dx, dz).wait_send()


def local(coeffs, counts, block_map, wrap):
    _, _, rows, parts, bands = coeffs.shape
    smem = pl.BlockSpec(memory_space=pltpu.SMEM)
    hbm = pl.BlockSpec(memory_space=pltpu.HBM)
    dma = pltpu.SemaphoreType.DMA
    out = pl.pallas_call(
        kernel,
        out_shape=jax.ShapeDtypeStruct((2, 16, NQ * LANE), jnp.float32),
        in_specs=[smem, hbm, hbm, hbm],
        out_specs=pl.BlockSpec(memory_space=pltpu.VMEM),
        scratch_shapes=[
            pltpu.VMEM((NQ, rows, parts, LANE), coeffs.dtype),
            pltpu.VMEM((3, 16, LANE), jnp.int32),
            pltpu.VMEM((16, LANE), jnp.int32),
            pltpu.VMEM((NS, LANE), jnp.int32),
            pltpu.SMEM((16, LANE), jnp.int32),
            pltpu.SMEM((NS, LANE), jnp.int32),
            pltpu.VMEM((NQ, NS, STEP // 2, 2, LANE), jnp.bfloat16),
            pltpu.VMEM((NQ, NS, STEP // 2, 2, LANE), jnp.bfloat16),
            pltpu.VMEM((NQ, NG * NR, STEP // 2, 2, LANE), jnp.bfloat16),
            pltpu.VMEM((1024, NS * STEP), jnp.bfloat16),
            pltpu.VMEM((GRP * STEP, LANE), jnp.bfloat16),
            pltpu.VMEM((NQ, 1024, LANE), jnp.float32),
            pltpu.VMEM((NQ, 512, LANE), jnp.float32),
            pltpu.VMEM((NQ, 256, LANE), jnp.float32),
            pltpu.VMEM((NQ - 1, NZ, 32, LANE), jnp.float32),
            pltpu.VMEM((NX * NZ, 32, LANE), jnp.float32),
            dma((NQ,)), dma((3,)), dma((2,)),
            dma((NQ, NS)), dma((NQ, NS)), dma((NQ, NG * NR)), dma((NQ, NG * NR)),
            dma((NQ,)), dma((NQ,)), dma((NQ,)), dma((NQ,)),
            dma((NQ, NZ)), dma((NQ, NZ)), dma((NX * NZ,)), dma((NX * NZ,)),
        ],
        compiler_params=pltpu.CompilerParams(
            collective_id=0, has_side_effects=True, vmem_limit_bytes=58 << 20),
    )(counts.reshape(-1), block_map.reshape(-1, LANE), wrap.reshape(-1, LANE), coeffs.reshape(rows, parts, bands))
    return out.transpose(1, 0, 2)[None, :, None]


def solution(mesh):
    placed = (P("ka", None, "ga", None, None), P(), P(), P())
    return jax.shard_map(
        local,
        mesh=mesh,
        in_specs=placed,
        out_specs=P("ka", "ga", None, None, None),
        check_vma=False,
    )
```

```python
import functools

import jax
import jax.numpy as jnp
from jax import lax
from jax.experimental import pallas as pl
from jax.experimental.pallas import tpu as pltpu
from jax.sharding import PartitionSpec as P

MESH = pl.DeviceIdType.MESH
BLK = 32
ROWS = 2 * BLK
CAP = 3
NS = 32
NZ = 8
NX = 2
LANE = 128
NQ = 4
GRP = 4
NG = NS // GRP
STEP = CAP * ROWS
AHEAD = 20
RELAYED = (1, 2)
DIRECT = (0, 3)
NR = len(RELAYED)
TOTAL = NQ * NG
RELAY_END = TOTAL - 3


def rem(a, b):
    return lax.rem(a, jnp.int32(b))


def div(a, b):
    return lax.div(a, jnp.int32(b))


def offset(grp, u):
    grp = rem(NG - grp, NG)
    d = div(grp + 1, 2)
    edge = 1 - div(rem(grp, 7) + 6, 7)
    odd = u % 2
    dz = d * (1 - 2 * odd * (1 - edge))
    dx = ((u + 1) // 2) % 2
    dc = edge * odd + (1 - edge) * rem(grp + 1, 2)
    return dz, dx, dc


def shifted(x, z, c, off, sign):
    dz, dx, dc = off
    return rem(x + dx, 2) * 16 + rem(z + sign * dz + 16, NZ) * 2 + rem(c + dc, 2)


def iota(rows, dim):
    return lax.broadcasted_iota(jnp.int32, (rows, LANE), dim)


def make_tables(k, g, counts, maps, send_tab, recv_tab):
    def place(hit):
        lane = iota(hit.shape[0], 1) & 63
        count = jnp.where(hit, 1, 0)
        for shift in (1, 2, 4, 8, 16, 32):
            count = count + jnp.where(lane >= shift, pltpu.roll(count, shift, 1), 0)
        return count

    def table(rows, columns):
        lane = iota(rows, 1)
        held = jnp.zeros((rows, LANE), jnp.int32)
        for n, (mask, value) in enumerate(columns):
            held = jnp.where(lane == n, jnp.sum(jnp.where(mask, value, 0), axis=1, keepdims=True), held)
        return held

    to_map = maps[0]
    hit = (to_map >> 6) == g
    rank = place(hit)
    half = iota(16, 1) >> 6
    value = to_map & 63
    send_tab[...] = table(16, [(hit & (rank == r + 1) & (half == h), value) for h in range(2) for r in range(CAP)])

    at = pl.ds(div(g, 2), 1)
    mine = maps[1, at, :]
    ids = iota(1, 1) & 63
    left_lim = counts[k] - (g * 64 + ids) * BLK
    right_lim = counts[rem(k + 1, 8)] - mine * BLK
    hit = (iota(NS, 0) == (mine >> 6)) & ((iota(NS, 1) >> 6) == rem(g, 2))
    rank = place(hit)
    recv_tab[...] = table(NS, [(hit & (rank == r + 1), v)
                               for v in (ids, maps[2, at, :], left_lim, right_lim) for r in range(CAP)])


def kernel(counts, block_map, wrap, coeffs, out, cin, maps, send_vec, recv_vec, send_tab, recv_tab,
           send, recv, relay, left, flat, acc, rs1, rs2, rs3, rs4, csem, map_sem, tab_sem,
           ssem, rsem, lsem, fsem, s1sem, r1sem, s2sem, r2sem, s3sem, r3sem, s4sem, r4sem):
    k = lax.axis_index("ka")
    g = lax.axis_index("ga")
    x, z, c = div(g, 16), rem(div(g, 2), NZ), rem(g, 2)
    k_to, k_from = rem(k + 7, 8), rem(k + 1, 8)
    core_peer = x * 16 + z * 2 + (1 - c)
    x_peer = (1 - x) * 16 + z * 2 + c

    def any_peer(dx, dz):
        return rem(x + dx, NX) * 16 + rem(z + dz, NZ) * 2 + c

    def map_rows(kk):
        return pl.ds(pl.multiple_of(kk * 16, 16), 16)

    fetches = [pltpu.make_async_copy(source.at[map_rows(kk)], maps.at[n], map_sem.at[n])
               for n, (source, kk) in enumerate(((block_map, k_to), (block_map, k), (wrap, k)))]
    copies = [pltpu.make_async_copy(coeffs.at[:, :, pl.ds(q * LANE, LANE)], cin.at[q], csem.at[q]) for q in range(NQ)]
    for copy in fetches + copies:
        copy.start()

    barrier = pltpu.get_barrier_semaphore()

    even = rem(k, 2) == 0
    k_relay = rem(k + 6, 8)
    flipped = (1 - x) * 16 + z * 2 + c

    def greet(kk, steps):
        def one(grp, carry):
            for u in steps:
                s = shifted(x, z, c, offset(grp, u), -1)
                pl.semaphore_signal(barrier, inc=1, device_id=(kk, s), device_id_type=MESH)
            return carry

        lax.fori_loop(0, NG, one, 0)

    greet(k_from, range(GRP))

    @pl.when(even)
    def _():
        def one(grp, carry):
            for u in RELAYED:
                s = x * 16 + rem(shifted(x, z, c, offset(grp, u), -1), 16)
                pl.semaphore_signal(barrier, inc=1, device_id=(rem(k + 2, 8), s), device_id_type=MESH)
            return carry

        lax.fori_loop(0, NG, one, 0)

    @pl.when(rem(k, 2) == 1)
    def _():
        pl.semaphore_signal(barrier, inc=1, device_id=(k_to, flipped), device_id_type=MESH)

    for peer in [core_peer] + [any_peer(dx, dz) for dx in range(NX) for dz in range(NZ) if dx or dz]:
        pl.semaphore_signal(barrier, inc=1, device_id=(k, peer), device_id_type=MESH)

    def stage(it):
        q, grp = div(it, NG), rem(it, NG)
        for u in range(GRP):
            t = shifted(x, z, c, offset(grp, u), 1)
            for r in range(CAP):
                blk = send_tab[div(t, 2), rem(t, 2) * CAP + r] & 63
                send[q, grp * GRP + u, r * BLK:(r + 1) * BLK] = cin[q, pl.ds(blk * BLK, BLK)]

    def exchange(it, u):
        q, grp = div(it, NG), rem(it, NG)
        j = grp * GRP + u
        t = shifted(x, z, c, offset(grp, u), 1)
        return pltpu.make_async_remote_copy(
            src_ref=send.at[q, j], dst_ref=recv.at[q, j], send_sem=ssem.at[q, j], recv_sem=rsem.at[q, j],
            device_id=(k_to, t), device_id_type=MESH)

    def to_relay(it, n):
        q, grp = div(it, NG), rem(it, NG)
        t = x * 16 + rem(shifted(x, z, c, offset(grp, RELAYED[n]), 1), 16)
        return pltpu.make_async_remote_copy(
            src_ref=send.at[q, grp * GRP + RELAYED[n]], dst_ref=relay.at[q, grp * NR + n],
            send_sem=ssem.at[q, grp * GRP + RELAYED[n]], recv_sem=lsem.at[q, grp * NR + n],
            device_id=(k_relay, t), device_id_type=MESH)

    def forward(it, n):
        q, grp = div(it, NG), rem(it, NG)
        j = grp * GRP + RELAYED[n]
        return pltpu.make_async_remote_copy(
            src_ref=relay.at[q, grp * NR + n], dst_ref=recv.at[q, j],
            send_sem=fsem.at[q, grp * NR + n], recv_sem=rsem.at[q, j],
            device_id=(k_from, flipped), device_id_type=MESH)

    def launch(it):
        @pl.when(even & (it < RELAY_END))
        def _():
            for n in range(NR):
                to_relay(it, n).start()

        @pl.when(jnp.logical_not(even & (it < RELAY_END)))
        def _():
            for u in RELAYED:
                exchange(it, u).start()

        for u in DIRECT:
            exchange(it, u).start()

    def pass_on(it):
        @pl.when(even & (it < RELAY_END))
        def _():
            for n in range(NR):
                to_relay(it, n).wait_recv()
                forward(it, n).start()

    row = lax.broadcasted_iota(jnp.int32, (2 * ROWS, 4 * ROWS), 0)
    col = lax.broadcasted_iota(jnp.int32, (2 * ROWS, 4 * ROWS), 1)
    left_lane = rem(div(row, 2), BLK)
    right_lane = rem(div(col, 2), BLK)
    first = row < ROWS
    same_slot = div(row, ROWS) == rem(div(col, ROWS), 2)
    straight = col < 2 * ROWS
    same_part = rem(row, 2) == rem(col, 2)
    sign = jnp.where(straight, jnp.where(same_part, 1.0, 0.0),
                     jnp.where(same_part, 0.0, jnp.where(rem(row, 2) == 0, 1.0, -1.0)))
    pattern = jnp.where(same_slot, sign, 0.0)

    def build(grp):
        for pair in range(GRP * CAP // 2):
            slots = []
            for h in range(2):
                u, r = divmod(2 * pair + h, CAP)
                s = shifted(x, z, c, offset(grp, u), -1)
                slots.append([recv_tab[s, n * CAP + r] for n in range(4)])
            (b0, w0, l0, r0), (b1, w1, l1, r1) = slots
            w = jnp.where(first, w0, w1)
            hit = left_lane == ((right_lane - w) & (BLK - 1))
            hit = hit & (left_lane < jnp.where(first, l0, l1)) & (right_lane < jnp.where(first, r0, r1))
            pick = jnp.where(hit, pattern, 0.0).astype(jnp.bfloat16)
            cols = pl.ds(pl.multiple_of(grp * (GRP * STEP) + pair * 2 * ROWS, LANE), 2 * ROWS)
            for q in range(NQ):
                held = jnp.concatenate([cin[q, pl.ds((b & 63) * BLK, BLK)].reshape(ROWS, LANE) for b in (b0, b1)], axis=0)
                moved = lax.dot_general(held, pick, (((0,), (0,)), ((), ())),
                                        preferred_element_type=jnp.float32).astype(jnp.bfloat16)
                for ii in range(8):
                    i = q * 8 + ii
                    ix, iz, ic = i // 16, (i // 2) % NZ, i % 2
                    base = ((ic * 2 + ix) * NZ + iz) * 32
                    part = moved[ii * 16:(ii + 1) * 16]
                    left[base:base + 16, cols] = part[:, :LANE]
                    left[base + 16:base + 32, cols] = part[:, LANE:]

    def multiply(it):
        q, grp = div(it, NG), rem(it, NG)
        for u in range(GRP):
            exchange(it, u).wait_recv()
        j0 = grp * GRP
        cols = pl.ds(pl.multiple_of(grp * (GRP * STEP), LANE), GRP * STEP)
        for u in range(GRP):
            flat[u * STEP:(u + 1) * STEP] = recv[q, j0 + u].reshape(STEP, LANE)
        part = 256

        def strip(owner, n):
            rows = pl.ds(pl.multiple_of(owner * 512 + n * part, part), part)
            val = jnp.dot(left[rows, cols], flat[...], preferred_element_type=jnp.float32)

            @pl.when(grp == 0)
            def _():
                acc[q, rows] = val

            @pl.when(grp > 0)
            def _():
                acc[q, rows] += val

        for n in range(2):
            strip(1 - c, n)

        @pl.when(grp == NG - 1)
        def _():
            to_core(q).start()

        for n in range(2):
            strip(c, n)

    def half(which):
        return pl.ds(pl.multiple_of(which * 512, 512), 512)

    def quarter(cc, xx):
        return pl.ds(pl.multiple_of(cc * 512 + xx * 256, 256), 256)

    def piece(cc, xx, zz):
        return pl.ds(pl.multiple_of(cc * 512 + xx * 256 + zz * 32, 32), 32)

    def to_core(q):
        return pltpu.make_async_remote_copy(
            src_ref=acc.at[q, half(1 - c)], dst_ref=rs1.at[q], send_sem=s1sem.at[q], recv_sem=r1sem.at[q],
            device_id=(k, core_peer), device_id_type=MESH)

    def to_x(q):
        return pltpu.make_async_remote_copy(
            src_ref=acc.at[q, quarter(c, 1 - x)], dst_ref=rs2.at[q], send_sem=s2sem.at[q], recv_sem=r2sem.at[q],
            device_id=(k, x_peer), device_id_type=MESH)

    def to_z(q, dz):
        return pltpu.make_async_remote_copy(
            src_ref=acc.at[q, piece(c, x, rem(z + dz, NZ))], dst_ref=rs3.at[q, dz],
            send_sem=s3sem.at[q, dz], recv_sem=r3sem.at[q, dz],
            device_id=(k, any_peer(0, dz)), device_id_type=MESH)

    def to_any(q, dx, dz):
        n = dx * NZ + dz
        return pltpu.make_async_remote_copy(
            src_ref=acc.at[q, piece(c, rem(x + dx, NX), rem(z + dz, NZ))], dst_ref=rs4.at[n],
            send_sem=s4sem.at[n], recv_sem=r4sem.at[n],
            device_id=(k, any_peer(dx, dz)), device_id_type=MESH)

    def after_core(q):
        to_core(q).wait_recv()
        acc[q, half(c)] += rs1[q]
        to_x(q).start()

    def after_x(q):
        to_x(q).wait_recv()
        acc[q, quarter(c, x)] += rs2[q]
        for dz in range(1, NZ):
            to_z(q, dz).start()

    def finish(q):
        total = acc[q, piece(c, x, z)]
        for dz in range(1, NZ):
            to_z(q, dz).wait_recv()
            total = total + rs3[q, dz]
        out[0, :, q * LANE:(q + 1) * LANE] = total[:16]
        out[1, :, q * LANE:(q + 1) * LANE] = total[16:]

    far_first = sorted(((dx, dz) for dx in range(NX) for dz in range(NZ) if dx or dz),
                       key=lambda p: -min(p[1], NZ - p[1]))

    def spread(q):
        to_core(q).wait_recv()
        acc[q, half(c)] += rs1[q]
        for dx, dz in far_first:
            to_any(q, dx, dz).start()

    def finish_last(q):
        total = acc[q, piece(c, x, z)]
        for dx, dz in reversed(far_first):
            to_any(q, dx, dz).wait_recv()
            total = total + rs4[dx * NZ + dz]
        out[0, :, q * LANE:(q + 1) * LANE] = total[:16]
        out[1, :, q * LANE:(q + 1) * LANE] = total[16:]

    for copy in fetches:
        copy.wait()
    make_tables(k, g, counts, maps, send_vec, recv_vec)
    tables = [pltpu.make_async_copy(vec, tab, tab_sem.at[n])
              for n, (vec, tab) in enumerate(((send_vec, send_tab), (recv_vec, recv_tab)))]
    for copy in tables:
        copy.start()
    for copy in tables + copies:
        copy.wait()
    stage(jnp.int32(0))
    pl.semaphore_wait(barrier, NS + NX * NZ + (1 - rem(k, 2)) * 17)

    def start(it, carry):
        launch(it)
        stage(it + 1)
        return carry

    lax.fori_loop(0, AHEAD, start, 0)

    def body(it, carry):
        q, grp = div(it, NG), rem(it, NG)

        @pl.when(it + AHEAD < TOTAL)
        def _():
            launch(it + AHEAD)

        @pl.when(it + AHEAD + 1 < TOTAL)
        def _():
            stage(it + AHEAD + 1)

        @pl.when(q == 0)
        def _():
            build(grp)

        @pl.when((q > 0) & (grp == 2))
        def _():
            after_core(q - 1)

        @pl.when((q > 0) & (grp == 4))
        def _():
            after_x(q - 1)

        pass_on(it)
        multiply(it)
        return carry

    lax.fori_loop(0, TOTAL, body, 0)
    last = NQ - 1
    spread(last)
    for q in range(last):
        finish(q)
    finish_last(last)

    def drain(it, carry):
        for u in range(GRP):
            exchange(it, u).wait_send()

        @pl.when(even & (it < RELAY_END))
        def _():
            for n in range(NR):
                forward(it, n).wait_send()

        return carry

    lax.fori_loop(0, TOTAL, drain, 0)
    for q in range(NQ):
        to_core(q).wait_send()
    for q in range(last):
        to_x(q).wait_send()
        for dz in range(1, NZ):
            to_z(q, dz).wait_send()
    for dx, dz in far_first:
        to_any(last, dx, dz).wait_send()


def local(coeffs, counts, block_map, wrap):
    _, _, rows, parts, bands = coeffs.shape
    smem = pl.BlockSpec(memory_space=pltpu.SMEM)
    hbm = pl.BlockSpec(memory_space=pltpu.HBM)
    dma = pltpu.SemaphoreType.DMA
    out = pl.pallas_call(
        kernel,
        out_shape=jax.ShapeDtypeStruct((2, 16, NQ * LANE), jnp.float32),
        in_specs=[smem, hbm, hbm, hbm],
        out_specs=pl.BlockSpec(memory_space=pltpu.VMEM),
        scratch_shapes=[
            pltpu.VMEM((NQ, rows, parts, LANE), coeffs.dtype),
            pltpu.VMEM((3, 16, LANE), jnp.int32),
            pltpu.VMEM((16, LANE), jnp.int32),
            pltpu.VMEM((NS, LANE), jnp.int32),
            pltpu.SMEM((16, LANE), jnp.int32),
            pltpu.SMEM((NS, LANE), jnp.int32),
            pltpu.VMEM((NQ, NS, STEP // 2, 2, LANE), jnp.bfloat16),
            pltpu.VMEM((NQ, NS, STEP // 2, 2, LANE), jnp.bfloat16),
            pltpu.VMEM((NQ, NG * NR, STEP // 2, 2, LANE), jnp.bfloat16),
            pltpu.VMEM((1024, NS * STEP), jnp.bfloat16),
            pltpu.VMEM((GRP * STEP, LANE), jnp.bfloat16),
            pltpu.VMEM((NQ, 1024, LANE), jnp.float32),
            pltpu.VMEM((NQ, 512, LANE), jnp.float32),
            pltpu.VMEM((NQ, 256, LANE), jnp.float32),
            pltpu.VMEM((NQ - 1, NZ, 32, LANE), jnp.float32),
            pltpu.VMEM((NX * NZ, 32, LANE), jnp.float32),
            dma((NQ,)), dma((3,)), dma((2,)),
            dma((NQ, NS)), dma((NQ, NS)), dma((NQ, NG * NR)), dma((NQ, NG * NR)),
            dma((NQ,)), dma((NQ,)), dma((NQ,)), dma((NQ,)),
            dma((NQ, NZ)), dma((NQ, NZ)), dma((NX * NZ,)), dma((NX * NZ,)),
        ],
        compiler_params=pltpu.CompilerParams(
            collective_id=0, has_side_effects=True, vmem_limit_bytes=58 << 20),
    )(counts.reshape(-1), block_map.reshape(-1, LANE), wrap.reshape(-1, LANE), coeffs.reshape(rows, parts, bands))
    return out.transpose(1, 0, 2)[None, :, None]


def solution(mesh):
    placed = (P("ka", None, "ga", None, None), P(), P(), P())
    return jax.shard_map(
        local,
        mesh=mesh,
        in_specs=placed,
        out_specs=P("ka", "ga", None, None, None),
        check_vma=False,
    )
```

```python
import functools

import jax
import jax.numpy as jnp
from jax import lax
from jax.experimental import pallas as pl
from jax.experimental.pallas import tpu as pltpu
from jax.sharding import PartitionSpec as P

MESH = pl.DeviceIdType.MESH
BLK = 32
ROWS = 2 * BLK
CAP = 3
NS = 32
NZ = 8
NX = 2
LANE = 128
NQ = 4
GRP = 4
NG = NS // GRP
STEP = CAP * ROWS
AHEAD = 23
RELAYED = (1, 2)
DIRECT = (0, 3)
NR = len(RELAYED)
TOTAL = NQ * NG
RELAY_END = TOTAL - 2


def rem(a, b):
    return lax.rem(a, jnp.int32(b))


def div(a, b):
    return lax.div(a, jnp.int32(b))


def offset(grp, u):
    grp = rem(NG - grp, NG)
    d = div(grp + 1, 2)
    edge = 1 - div(rem(grp, 7) + 6, 7)
    odd = u % 2
    dz = d * (1 - 2 * odd * (1 - edge))
    dx = ((u + 1) // 2) % 2
    dc = edge * odd + (1 - edge) * rem(grp + 1, 2)
    return dz, dx, dc


def shifted(x, z, c, off, sign):
    dz, dx, dc = off
    return rem(x + dx, 2) * 16 + rem(z + sign * dz + 16, NZ) * 2 + rem(c + dc, 2)


def iota(rows, dim):
    return lax.broadcasted_iota(jnp.int32, (rows, LANE), dim)


def make_tables(k, g, counts, maps, send_tab, recv_tab):
    def place(hit):
        lane = iota(hit.shape[0], 1) & 63
        count = jnp.where(hit, 1, 0)
        for shift in (1, 2, 4, 8, 16, 32):
            count = count + jnp.where(lane >= shift, pltpu.roll(count, shift, 1), 0)
        return count

    def table(rows, columns):
        lane = iota(rows, 1)
        held = jnp.zeros((rows, LANE), jnp.int32)
        for n, (mask, value) in enumerate(columns):
            held = jnp.where(lane == n, jnp.sum(jnp.where(mask, value, 0), axis=1, keepdims=True), held)
        return held

    to_map = maps[0]
    hit = (to_map >> 6) == g
    rank = place(hit)
    half = iota(16, 1) >> 6
    value = to_map & 63
    send_tab[...] = table(16, [(hit & (rank == r + 1) & (half == h), value) for h in range(2) for r in range(CAP)])

    at = pl.ds(div(g, 2), 1)
    mine = maps[1, at, :]
    ids = iota(1, 1) & 63
    left_lim = counts[k] - (g * 64 + ids) * BLK
    right_lim = counts[rem(k + 1, 8)] - mine * BLK
    hit = (iota(NS, 0) == (mine >> 6)) & ((iota(NS, 1) >> 6) == rem(g, 2))
    rank = place(hit)
    recv_tab[...] = table(NS, [(hit & (rank == r + 1), v)
                               for v in (ids, maps[2, at, :], left_lim, right_lim) for r in range(CAP)])


def kernel(counts, block_map, wrap, coeffs, out, cin, cin0, maps, send_vec, recv_vec, send_tab, recv_tab,
           send, recv, relay, left, flat, acc, rs1, rs2, rs3, rs4, csem, map_sem, tab_sem,
           ssem, rsem, lsem, fsem, s1sem, r1sem, s2sem, r2sem, s3sem, r3sem, s4sem, r4sem):
    k = lax.axis_index("ka")
    g = lax.axis_index("ga")
    x, z, c = div(g, 16), rem(div(g, 2), NZ), rem(g, 2)
    k_to, k_from = rem(k + 7, 8), rem(k + 1, 8)
    core_peer = x * 16 + z * 2 + (1 - c)
    x_peer = (1 - x) * 16 + z * 2 + c

    def any_peer(dx, dz):
        return rem(x + dx, NX) * 16 + rem(z + dz, NZ) * 2 + c

    def map_rows(kk):
        return pl.ds(pl.multiple_of(kk * 16, 16), 16)

    fetches = [pltpu.make_async_copy(source.at[map_rows(kk)], maps.at[n], map_sem.at[n])
               for n, (source, kk) in enumerate(((block_map, k_to), (block_map, k), (wrap, k)))]
    copies = [pltpu.make_async_copy(coeffs.at[:, :, pl.ds(q * LANE, LANE)], dst, csem.at[n])
              for n, (q, dst) in enumerate([(0, cin0)] + [(q, cin.at[q]) for q in range(NQ)])]
    for copy in fetches + copies:
        copy.start()

    barrier = pltpu.get_barrier_semaphore()

    even = rem(k, 2) == 0
    k_relay = rem(k + 6, 8)
    flipped = (1 - x) * 16 + z * 2 + c

    def greet(kk, steps):
        def one(grp, carry):
            for u in steps:
                s = shifted(x, z, c, offset(grp, u), -1)
                pl.semaphore_signal(barrier, inc=1, device_id=(kk, s), device_id_type=MESH)
            return carry

        lax.fori_loop(0, NG, one, 0)

    greet(k_from, range(GRP))

    @pl.when(even)
    def _():
        def one(grp, carry):
            for u in RELAYED:
                s = x * 16 + rem(shifted(x, z, c, offset(grp, u), -1), 16)
                pl.semaphore_signal(barrier, inc=1, device_id=(rem(k + 2, 8), s), device_id_type=MESH)
            return carry

        lax.fori_loop(0, NG, one, 0)

    @pl.when(rem(k, 2) == 1)
    def _():
        pl.semaphore_signal(barrier, inc=1, device_id=(k_to, flipped), device_id_type=MESH)

    for peer in [core_peer] + [any_peer(dx, dz) for dx in range(NX) for dz in range(NZ) if dx or dz]:
        pl.semaphore_signal(barrier, inc=1, device_id=(k, peer), device_id_type=MESH)

    def stage(it, held=None):
        q, grp = div(it, NG), rem(it, NG)
        for u in range(GRP):
            t = shifted(x, z, c, offset(grp, u), 1)
            for r in range(CAP):
                blk = send_tab[div(t, 2), rem(t, 2) * CAP + r] & 63
                rows = pl.ds(blk * BLK, BLK)
                send[q, grp * GRP + u, r * BLK:(r + 1) * BLK] = cin[q, rows] if held is None else held[rows]

    def exchange(it, u):
        q, grp = div(it, NG), rem(it, NG)
        j = grp * GRP + u
        t = shifted(x, z, c, offset(grp, u), 1)
        return pltpu.make_async_remote_copy(
            src_ref=send.at[q, j], dst_ref=recv.at[q, j], send_sem=ssem.at[q, j], recv_sem=rsem.at[q, j],
            device_id=(k_to, t), device_id_type=MESH)

    def to_relay(it, n):
        q, grp = div(it, NG), rem(it, NG)
        t = x * 16 + rem(shifted(x, z, c, offset(grp, RELAYED[n]), 1), 16)
        return pltpu.make_async_remote_copy(
            src_ref=send.at[q, grp * GRP + RELAYED[n]], dst_ref=relay.at[q, grp * NR + n],
            send_sem=ssem.at[q, grp * GRP + RELAYED[n]], recv_sem=lsem.at[q, grp * NR + n],
            device_id=(k_relay, t), device_id_type=MESH)

    def forward(it, n):
        q, grp = div(it, NG), rem(it, NG)
        j = grp * GRP + RELAYED[n]
        return pltpu.make_async_remote_copy(
            src_ref=relay.at[q, grp * NR + n], dst_ref=recv.at[q, j],
            send_sem=fsem.at[q, grp * NR + n], recv_sem=rsem.at[q, j],
            device_id=(k_from, flipped), device_id_type=MESH)

    def arrival(q, j):
        return pltpu.make_async_remote_copy(
            src_ref=send.at[q, j], dst_ref=recv.at[q, j], send_sem=ssem.at[q, j], recv_sem=rsem.at[q, j],
            device_id=(k_to, g), device_id_type=MESH)

    def launch(it):
        @pl.when(even & (it < RELAY_END))
        def _():
            for n in range(NR):
                to_relay(it, n).start()

        @pl.when(jnp.logical_not(even & (it < RELAY_END)))
        def _():
            for u in RELAYED:
                exchange(it, u).start()

        for u in DIRECT:
            exchange(it, u).start()

    def pass_on(it):
        @pl.when(even & (it < RELAY_END))
        def _():
            for n in range(NR):
                to_relay(it, n).wait_recv()
                forward(it, n).start()

    row = lax.broadcasted_iota(jnp.int32, (2 * ROWS, 4 * ROWS), 0)
    col = lax.broadcasted_iota(jnp.int32, (2 * ROWS, 4 * ROWS), 1)
    left_lane = rem(div(row, 2), BLK)
    right_lane = rem(div(col, 2), BLK)
    first = row < ROWS
    same_slot = div(row, ROWS) == rem(div(col, ROWS), 2)
    straight = col < 2 * ROWS
    same_part = rem(row, 2) == rem(col, 2)
    sign = jnp.where(straight, jnp.where(same_part, 1.0, 0.0),
                     jnp.where(same_part, 0.0, jnp.where(rem(row, 2) == 0, 1.0, -1.0)))
    pattern = jnp.where(same_slot, sign, 0.0)

    def build(grp):
        for pair in range(GRP * CAP // 2):
            slots = []
            for h in range(2):
                u, r = divmod(2 * pair + h, CAP)
                s = shifted(x, z, c, offset(grp, u), -1)
                slots.append([recv_tab[s, n * CAP + r] for n in range(4)])
            (b0, w0, l0, r0), (b1, w1, l1, r1) = slots
            w = jnp.where(first, w0, w1)
            hit = left_lane == ((right_lane - w) & (BLK - 1))
            hit = hit & (left_lane < jnp.where(first, l0, l1)) & (right_lane < jnp.where(first, r0, r1))
            pick = jnp.where(hit, pattern, 0.0).astype(jnp.bfloat16)
            cols = pl.ds(pl.multiple_of(grp * (GRP * STEP) + pair * 2 * ROWS, LANE), 2 * ROWS)
            for q in range(NQ):
                held = jnp.concatenate([cin[q, pl.ds((b & 63) * BLK, BLK)].reshape(ROWS, LANE) for b in (b0, b1)], axis=0)
                moved = lax.dot_general(held, pick, (((0,), (0,)), ((), ())),
                                        preferred_element_type=jnp.float32).astype(jnp.bfloat16)
                for ii in range(8):
                    i = q * 8 + ii
                    ix, iz, ic = i // 16, (i // 2) % NZ, i % 2
                    base = ((ic * 2 + ix) * NZ + iz) * 32
                    part = moved[ii * 16:(ii + 1) * 16]
                    left[base:base + 16, cols] = part[:, :LANE]
                    left[base + 16:base + 32, cols] = part[:, LANE:]

    def multiply(it):
        q, grp = div(it, NG), rem(it, NG)
        cols = pl.ds(pl.multiple_of(grp * (GRP * STEP), LANE), GRP * STEP)
        part = 256
        for u in range(GRP):
            j = grp * GRP + u
            arrival(q, j).wait_recv()
            flat[u * STEP:(u + 1) * STEP] = recv[q, j].reshape(STEP, LANE)

        def strips(owner):
            def strip(n, carry):
                rows = pl.ds(pl.multiple_of(owner * 512 + n * part, part), part)
                val = jnp.dot(left[rows, cols], flat[...], preferred_element_type=jnp.float32)

                @pl.when(grp == 0)
                def _():
                    acc[q, rows] = val

                @pl.when(grp > 0)
                def _():
                    acc[q, rows] += val

                return carry

            lax.fori_loop(0, 512 // part, strip, 0)

        strips(1 - c)

        @pl.when(grp == NG - 1)
        def _():
            to_core(q).start()

        strips(c)

    def half(which):
        return pl.ds(pl.multiple_of(which * 512, 512), 512)

    def quarter(cc, xx):
        return pl.ds(pl.multiple_of(cc * 512 + xx * 256, 256), 256)

    def piece(cc, xx, zz):
        return pl.ds(pl.multiple_of(cc * 512 + xx * 256 + zz * 32, 32), 32)

    def to_core(q):
        return pltpu.make_async_remote_copy(
            src_ref=acc.at[q, half(1 - c)], dst_ref=rs1.at[q], send_sem=s1sem.at[q], recv_sem=r1sem.at[q],
            device_id=(k, core_peer), device_id_type=MESH)

    def to_x(q):
        return pltpu.make_async_remote_copy(
            src_ref=acc.at[q, quarter(c, 1 - x)], dst_ref=rs2.at[q], send_sem=s2sem.at[q], recv_sem=r2sem.at[q],
            device_id=(k, x_peer), device_id_type=MESH)

    def to_z(q, dz):
        return pltpu.make_async_remote_copy(
            src_ref=acc.at[q, piece(c, x, rem(z + dz, NZ))], dst_ref=rs3.at[q, dz],
            send_sem=s3sem.at[q, dz], recv_sem=r3sem.at[q, dz],
            device_id=(k, any_peer(0, dz)), device_id_type=MESH)

    def to_any(q, dx, dz):
        n = dx * NZ + dz
        return pltpu.make_async_remote_copy(
            src_ref=acc.at[q, piece(c, rem(x + dx, NX), rem(z + dz, NZ))], dst_ref=rs4.at[n],
            send_sem=s4sem.at[n], recv_sem=r4sem.at[n],
            device_id=(k, any_peer(dx, dz)), device_id_type=MESH)

    def after_core(q):
        to_core(q).wait_recv()
        acc[q, half(c)] += rs1[q]
        to_x(q).start()

    def after_x(q):
        to_x(q).wait_recv()
        acc[q, quarter(c, x)] += rs2[q]
        for dz in range(1, NZ):
            to_z(q, dz).start()

    def finish(q):
        total = acc[q, piece(c, x, z)]
        for dz in range(1, NZ):
            to_z(q, dz).wait_recv()
            total = total + rs3[q, dz]
        out[0, :, q * LANE:(q + 1) * LANE] = total[:16]
        out[1, :, q * LANE:(q + 1) * LANE] = total[16:]

    far_first = sorted(((dx, dz) for dx in range(NX) for dz in range(NZ) if dx or dz),
                       key=lambda p: -min(p[1], NZ - p[1]))

    def spread(q):
        to_core(q).wait_recv()
        acc[q, half(c)] += rs1[q]
        for dx, dz in far_first:
            to_any(q, dx, dz).start()

    def finish_last(q):
        total = acc[q, piece(c, x, z)]
        for dx, dz in reversed(far_first):
            to_any(q, dx, dz).wait_recv()
            total = total + rs4[dx * NZ + dz]
        out[0, :, q * LANE:(q + 1) * LANE] = total[:16]
        out[1, :, q * LANE:(q + 1) * LANE] = total[16:]

    for copy in fetches:
        copy.wait()
    make_tables(k, g, counts, maps, send_vec, recv_vec)
    tables = [pltpu.make_async_copy(vec, tab, tab_sem.at[n])
              for n, (vec, tab) in enumerate(((send_vec, send_tab), (recv_vec, recv_tab)))]
    for copy in tables:
        copy.start()
    for copy in tables + copies[:1]:
        copy.wait()
    stage(jnp.int32(0), cin0)
    pl.semaphore_wait(barrier, NS + NX * NZ + (1 - rem(k, 2)) * 17)

    def start(it, carry, held=None):
        launch(it)
        stage(it + 1, held)
        return carry

    lax.fori_loop(0, NG - 1, functools.partial(start, held=cin0), 0)
    for copy in copies[1:]:
        copy.wait()
    lax.fori_loop(NG - 1, AHEAD, start, 0)

    def body(it, carry):
        q, grp = div(it, NG), rem(it, NG)

        @pl.when(it + AHEAD < TOTAL)
        def _():
            launch(it + AHEAD)

        @pl.when(it + AHEAD + 1 < TOTAL)
        def _():
            stage(it + AHEAD + 1)

        @pl.when(q == 0)
        def _():
            build(grp)

        @pl.when((q > 0) & (grp == 2))
        def _():
            after_core(q - 1)

        @pl.when((q > 0) & (grp == 4))
        def _():
            after_x(q - 1)

        pass_on(it)
        multiply(it)
        return carry

    lax.fori_loop(0, TOTAL, body, 0)
    last = NQ - 1
    spread(last)
    for q in range(last):
        finish(q)
    finish_last(last)

    def drain(it, carry):
        for u in range(GRP):
            exchange(it, u).wait_send()

        @pl.when(even & (it < RELAY_END))
        def _():
            for n in range(NR):
                forward(it, n).wait_send()

        return carry

    lax.fori_loop(0, TOTAL, drain, 0)
    for q in range(NQ):
        to_core(q).wait_send()
    for q in range(last):
        to_x(q).wait_send()
        for dz in range(1, NZ):
            to_z(q, dz).wait_send()
    for dx, dz in far_first:
        to_any(last, dx, dz).wait_send()


def local(coeffs, counts, block_map, wrap):
    _, _, rows, parts, bands = coeffs.shape
    smem = pl.BlockSpec(memory_space=pltpu.SMEM)
    hbm = pl.BlockSpec(memory_space=pltpu.HBM)
    dma = pltpu.SemaphoreType.DMA
    out = pl.pallas_call(
        kernel,
        out_shape=jax.ShapeDtypeStruct((2, 16, NQ * LANE), jnp.float32),
        in_specs=[smem, hbm, hbm, hbm],
        out_specs=pl.BlockSpec(memory_space=pltpu.VMEM),
        scratch_shapes=[
            pltpu.VMEM((NQ, rows, parts, LANE), coeffs.dtype),
            pltpu.VMEM((rows, parts, LANE), coeffs.dtype),
            pltpu.VMEM((3, 16, LANE), jnp.int32),
            pltpu.VMEM((16, LANE), jnp.int32),
            pltpu.VMEM((NS, LANE), jnp.int32),
            pltpu.SMEM((16, LANE), jnp.int32),
            pltpu.SMEM((NS, LANE), jnp.int32),
            pltpu.VMEM((NQ, NS, STEP // 2, 2, LANE), jnp.bfloat16),
            pltpu.VMEM((NQ, NS, STEP // 2, 2, LANE), jnp.bfloat16),
            pltpu.VMEM((NQ, NG * NR, STEP // 2, 2, LANE), jnp.bfloat16),
            pltpu.VMEM((1024, NS * STEP), jnp.bfloat16),
            pltpu.VMEM((GRP * STEP, LANE), jnp.bfloat16),
            pltpu.VMEM((NQ, 1024, LANE), jnp.float32),
            pltpu.VMEM((NQ, 512, LANE), jnp.float32),
            pltpu.VMEM((NQ, 256, LANE), jnp.float32),
            pltpu.VMEM((NQ - 1, NZ, 32, LANE), jnp.float32),
            pltpu.VMEM((NX * NZ, 32, LANE), jnp.float32),
            dma((NQ + 1,)), dma((3,)), dma((2,)),
            dma((NQ, NS)), dma((NQ, NS)), dma((NQ, NG * NR)), dma((NQ, NG * NR)),
            dma((NQ,)), dma((NQ,)), dma((NQ,)), dma((NQ,)),
            dma((NQ, NZ)), dma((NQ, NZ)), dma((NX * NZ,)), dma((NX * NZ,)),
        ],
        compiler_params=pltpu.CompilerParams(
            collective_id=0, has_side_effects=True, vmem_limit_bytes=58 << 20),
    )(counts.reshape(-1), block_map.reshape(-1, LANE), wrap.reshape(-1, LANE), coeffs.reshape(rows, parts, bands))
    return out.transpose(1, 0, 2)[None, :, None]


def solution(mesh):
    placed = (P("ka", None, "ga", None, None), P(), P(), P())
    return jax.shard_map(
        local,
        mesh=mesh,
        in_specs=placed,
        out_specs=P("ka", "ga", None, None, None),
        check_vma=False,
    )
```
